128 devices in a mesh: layer: 32 (over x, z, y_hi), width: 4 (over y_lo, core).
Axes of the slice: x: 4, y: 4 (y_hi: 2, y_lo: 2; y = y_hi * 2 + y_lo), z: 4, core: 2. Of those that a mesh axis runs over, the one named last changes fastest.
Arguments:
- mlp_inputs: bfloat16 [32, 768, 4096], P('layer', None, 'width'), may hold values from -6 to 6
- mlp_outputs: bfloat16 [32, 768, 4096], P('layer', None, 'width'), may hold values from -6 to 6
- encoders: bfloat16 [32, 4096, 128], P('layer', 'width'), may hold values from -0.09375 to 0.09375
- encoder_bias: float32 [32, 128], P('layer'), may hold values from -0.5 to 0
- decoders: bfloat16 [32, 32, 128, 4096], P('layer', None, None, 'width'), may hold values from -0.1875 to 0.1875
Outputs:
- loss_mean: float32 [], replicated
- grad_encoders: bfloat16 [32, 4096, 128], P('layer', 'width')
- grad_encoder_bias: float32 [32, 128], P('layer')
- grad_decoders: bfloat16 [32, 32, 128, 4096], P('layer', None, None, 'width')
The draws below stay inside these ranges and needn't reach their ends.
All inputs are finite; a program needn't handle non-finite values.
Results may differ from the reference program's by a relative error of at most 0.0055.
Values may be sent and summed in bfloat16 or wider, within the bound.
No kernel may reach another device: no remote copies, remote signals or barrier semaphores. Data moves between devices by JAX's collectives and lax.ppermute only.
A program may use at most 128 MiB of HBM per device.

```python
import jax
import jax.numpy as jnp
from jax import lax

D = 4096
LATENT_WIDTH = 128
TOKENS = 768
DEPTH_TOTAL = 32


def steps_of(key, dims, cuts, least, top_value):
    def one(axis_at, parts):
        draws = jax.random.uniform(jax.random.fold_in(jax.random.fold_in(key, 6), axis_at), (parts,), jnp.float32, least / len(cuts), top_value / len(cuts))
        return jnp.repeat(jnp.exp(draws), dims[axis_at] // parts).reshape((-1,) + (1,) * (len(dims) - axis_at - 1))

    loudness = one(*cuts[0])
    for cut in cuts[1:]:
        loudness = loudness * one(*cut)
    return loudness


def gaussian(rng, dims, deviation, limit, shards=(), kind=jnp.bfloat16):
    values = deviation * jax.random.normal(rng, dims, jnp.float32)
    if shards:
        values = values * steps_of(rng, dims, shards, -0.22, 0.18)
    return jnp.clip(values, -limit, limit).astype(kind)


def setup_inputs(seed: int = 0) -> dict:
    splits = jax.random.split(jax.random.key(seed), 6)
    mlp_inputs = gaussian(splits[0], (DEPTH_TOTAL, TOKENS, D), 1.0, 6.0, ((0, 32), (2, 4)))
    mlp_outputs = gaussian(splits[1], (DEPTH_TOTAL, TOKENS, D), 1.0, 6.0, ((0, 32), (2, 4)))
    encoders = gaussian(splits[2], (DEPTH_TOTAL, D, LATENT_WIDTH), D ** -0.5, 0.09375, ((0, 32), (1, 4)))
    encoder_bias = jnp.clip(-0.5 + 0.5 * jax.random.uniform(splits[3], (DEPTH_TOTAL, LATENT_WIDTH), jnp.float32) ** steps_of(splits[3], (DEPTH_TOTAL, LATENT_WIDTH), ((0, 32),), -0.2, 0.2), -0.5, 0.0)
    decoders = gaussian(splits[4], (DEPTH_TOTAL, DEPTH_TOTAL, LATENT_WIDTH, D), (LATENT_WIDTH * 8) ** -0.5, 0.1875, ((0, 32), (3, 4)))
    return dict(mlp_inputs=mlp_inputs, mlp_outputs=mlp_outputs, encoders=encoders, encoder_bias=encoder_bias, decoders=decoders)


sparsity = 8.0

def reference(mlp_inputs, mlp_outputs, encoders, encoder_bias, decoders):
    position_vectors = mlp_inputs.shape[1]

    def encode(pair):
        return jnp.dot(pair[0], pair[1], preferred_element_type=jnp.float32)
    potential = lax.map(encode, (mlp_inputs, encoders)) + encoder_bias[:, None, :]
    nonzero_latents = jnp.maximum(potential, 0.0)
    positive_indicator = nonzero_latents.astype(jnp.bfloat16)
    merged_positions = jnp.transpose(positive_indicator, (1, 0, 2)).reshape(position_vectors, DEPTH_TOTAL * LATENT_WIDTH)
    sources = jnp.arange(DEPTH_TOTAL, dtype=jnp.int32)

    def target_step(running, inputs):
        target, decoder, wanted = inputs
        columns = jnp.repeat(sources <= target, LATENT_WIDTH)
        masked = merged_positions * columns.astype(jnp.bfloat16)[None, :]
        weights = decoder.reshape(DEPTH_TOTAL * LATENT_WIDTH, D)
        rebuilt = jnp.dot(masked, weights, preferred_element_type=jnp.float32)
        misfit = rebuilt - wanted.astype(jnp.float32)
        signal = (misfit / position_vectors).astype(jnp.bfloat16)
        backward = jnp.dot(signal, weights.T, preferred_element_type=jnp.float32)
        backward = backward * columns.astype(jnp.float32)[None, :]
        grad_block = jnp.dot(masked.T, signal, preferred_element_type=jnp.float32)
        grad_block = grad_block.astype(jnp.bfloat16).reshape(DEPTH_TOTAL, LATENT_WIDTH, D)
        return (running + backward, (0.5 * jnp.sum(misfit * misfit), grad_block))
    start_total = jnp.zeros((position_vectors, DEPTH_TOTAL * LATENT_WIDTH), jnp.float32)
    targets = jnp.arange(DEPTH_TOTAL, dtype=jnp.int32)
    summed, outputs = lax.scan(target_step, start_total, (targets, decoders, mlp_outputs))
    squares, grad_decoders = outputs
    feature_grad = jnp.transpose(summed.reshape(position_vectors, DEPTH_TOTAL, LATENT_WIDTH), (1, 0, 2))
    delta = (feature_grad + sparsity / position_vectors) * (potential > 0).astype(jnp.float32)

    def encoder_grad(pair):
        return lax.dot_general(pair[0], pair[1].astype(jnp.bfloat16), (((0,), (0,)), ((), ())), preferred_element_type=jnp.float32).astype(jnp.bfloat16)
    grad_encoders = lax.map(encoder_grad, (mlp_inputs, delta))
    grad_encoder_bias = lax.optimization_barrier(jnp.sum(delta, axis=1))
    loss_mean = (jnp.sum(squares) + sparsity * jnp.sum(nonzero_latents)) / (position_vectors * D * DEPTH_TOTAL)
    return (loss_mean, grad_encoders, grad_encoder_bias, grad_decoders)
```

```python
import jax
import jax.numpy as jnp
from jax import lax
from jax.sharding import Mesh
from jax.sharding import PartitionSpec as P

AXES = ("x", "z", "yh", "yl", "c")
LAYER = ("x", "z", "yh")
WIDTH = ("yl", "c")
CHIPS = ("x", "z", "yh", "yl")
SWAP = [(0, 1), (1, 0)]
EXTRA = 16

sparsity = 8.0


def swapped(array, axis):
    return lax.ppermute(array, axis, SWAP)


def halves(array, axis, dim=0):
    half = array.shape[dim] // 2
    own = lax.axis_index(axis)
    mine = lax.dynamic_slice_in_dim(array, own * half, half, dim)
    theirs = lax.dynamic_slice_in_dim(array, (1 - own) * half, half, dim)
    return mine, theirs


def joined(array, axis):
    other = swapped(array, axis)
    first = lax.axis_index(axis) == 0
    return jnp.concatenate([jnp.where(first, array, other), jnp.where(first, other, array)], axis=0)


def exchanged(blocks):
    return lax.all_to_all(blocks, CHIPS, 0, 0, tiled=True)


def two_parts(value):
    high = value.astype(jnp.bfloat16)
    return high, (value - high.astype(jnp.float32)).astype(jnp.bfloat16)


def per_device(mlp_inputs, mlp_outputs, encoders, encoder_bias, decoders):
    f32, bf16 = jnp.float32, jnp.bfloat16
    inputs = mlp_inputs[0]
    tokens = inputs.shape[0]
    half, quarter = tokens // 2, tokens // 4
    width = inputs.shape[1] * lax.axis_size(WIDTH)
    layers = lax.axis_size(LAYER)
    chips = lax.axis_size(CHIPS)
    own_layer = lax.axis_index(LAYER)

    weights = decoders[0]
    weights_other = swapped(weights, "c")
    wanted, wanted_sent = halves(mlp_outputs[0], "c")
    wanted_other = swapped(wanted_sent, "c")

    partial = jnp.dot(inputs, encoders[0], preferred_element_type=f32)
    mine, theirs = halves(partial, "c")
    partial = mine + swapped(theirs, "c")
    mine, theirs = halves(partial, "yl")
    potential = mine + swapped(theirs, "yl") + encoder_bias[0][None, :]
    active = jnp.maximum(potential, 0.0)
    firing = active.astype(bf16)

    features = exchanged(jnp.broadcast_to(firing[None], (chips, *firing.shape)))
    features = features.reshape(layers, half, -1)
    allowed = (jnp.arange(layers) <= own_layer)[:, None, None]
    masked = features * allowed.astype(bf16)
    masked_other = swapped(masked, "c")

    def forward(w, target):
        rebuilt = jnp.einsum("ltf,lfd->td", masked, w, preferred_element_type=f32)
        return rebuilt - target.astype(f32)

    misfit = forward(weights, wanted)
    misfit_other = forward(weights_other, wanted_other)
    signal = (misfit / tokens).astype(bf16)
    signal_other = (misfit_other / tokens).astype(bf16)
    signal_here = swapped(signal_other, "c")

    squares = jnp.sum(misfit * misfit) + jnp.sum(misfit_other * misfit_other)
    loss = 0.5 * squares + sparsity * jnp.sum(active)

    terms = jnp.einsum("td,lfd->ltf", signal, weights, preferred_element_type=f32)
    terms = terms + jnp.einsum("td,lfd->ltf", signal_other, weights_other, preferred_element_type=f32)
    terms = (terms * allowed.astype(f32)).astype(bf16).reshape(chips, quarter, -1)
    high, low = two_parts(jnp.full((1, EXTRA // 2, terms.shape[2]), loss))
    note = jnp.broadcast_to(jnp.concatenate([high, low], axis=1), (chips, EXTRA, terms.shape[2]))
    arrived = exchanged(jnp.concatenate([terms, note], axis=1)).astype(f32)
    total = jnp.sum(arrived, axis=0)
    feature_grad = total[:quarter]
    delta = jnp.where(potential > 0, feature_grad + sparsity / tokens, 0.0).astype(bf16)

    loss = total[quarter : quarter + 1] + total[quarter + EXTRA // 2 : quarter + EXTRA // 2 + 1]
    loss = loss + swapped(loss, "c")
    loss_mean = loss[0, 0] / (tokens * width * layers)

    delta = joined(joined(delta, "yl"), "c")
    contract = (((0,), (0,)), ((), ()))
    grad_encoder = lax.dot_general(inputs, delta, contract, preferred_element_type=f32).astype(bf16)
    grad_bias = jnp.sum(delta.astype(f32), axis=0)

    fired = jnp.concatenate([masked, masked_other], axis=1)
    pulls = jnp.concatenate([signal, signal_here], axis=0)
    grad_decoder = jnp.einsum("ltf,td->lfd", fired, pulls, preferred_element_type=f32).astype(bf16)
    return (loss_mean, grad_encoder[None], grad_bias[None], grad_decoder[None])


def solution(mesh):
    finer = Mesh(mesh.devices.reshape(4, 4, 2, 2, 2), AXES)
    placed = (
        P(LAYER, None, WIDTH),
        P(LAYER, None, WIDTH),
        P(LAYER, WIDTH, None),
        P(LAYER, None),
        P(LAYER, None, None, WIDTH),
    )
    return jax.shard_map(
        per_device,
        mesh=finer,
        in_specs=placed,
        out_specs=(P(), P(LAYER, WIDTH, None), P(LAYER, None), P(LAYER, None, None, WIDTH)),
        check_vma=False,
    )
```

```python
import functools
import itertools

import jax
import jax.numpy as jnp
from jax import lax
from jax.experimental import pallas as pl
from jax.experimental.pallas import tpu as pltpu
from jax.sharding import Mesh
from jax.sharding import PartitionSpec as P

AXES = ("x", "z", "yh", "yl", "c")
LAYER = ("x", "z", "yh")
WIDTH = ("yl", "c")
SWAP = [(0, 1), (1, 0)]
RING = 4
EXTRA = 16
INTERPRET = False

sparsity = 8.0
f32, bf16 = jnp.float32, jnp.bfloat16


def flat(x, z, y, c):
    return ((x % RING * RING + z % RING) * RING + y % RING) * 2 + c


def toward(shift, back=False):
    pairs = []
    for x, z, y, c in itertools.product(range(RING), range(RING), range(RING), range(2)):
        if c == 0:
            there = {1: (x + 1, z, y), 3: (x - 1, z, y), 2: (x, z, y + 1)}[shift]
        else:
            there = {1: (x, z + 1, y), 3: (x, z - 1, y), 2: (x, z, y - 1)}[shift]
        pair = (flat(x, z, y, c), flat(*there, c))
        pairs.append(pair[::-1] if back else pair)
    return pairs


COSETS = [
    [flat(x, f - x - 2 * yl, 2 * yh + yl, c) for x in range(RING) for yh in range(2) for yl in range(2)]
    for f in range(RING)
    for c in range(2)
]


def sent(array, shift, back=False):
    return lax.ppermute(array, AXES, toward(shift, back))


def in_coset(blocks):
    return lax.all_to_all(blocks, AXES, 0, 0, axis_index_groups=COSETS, tiled=True)


def swapped(array, axis):
    return lax.ppermute(array, axis, SWAP)


def halves(array, axis, dim=0):
    half = array.shape[dim] // 2
    own = lax.axis_index(axis)
    mine = lax.dynamic_slice_in_dim(array, own * half, half, dim)
    theirs = lax.dynamic_slice_in_dim(array, (1 - own) * half, half, dim)
    return mine, theirs


def pair_of(place, offset, turn, x):
    return RING * x + lax.rem(place[0] + offset + 2 * turn + RING - x, RING)


ORDER = tuple(itertools.product(range(2), range(RING)))
CHIP = pl.BlockSpec(memory_space=pltpu.VMEM)
SCALARS = pl.BlockSpec(memory_space=pltpu.SMEM)
FAR = pl.BlockSpec(memory_space=pltpu.HBM)


def near(array):
    return array if INTERPRET else pltpu.with_memory_space_constraint(array, pltpu.VMEM)


def far(array):
    return array if INTERPRET else pltpu.with_memory_space_constraint(array, pltpu.HBM)


def near_out(shape, kind):
    return jax.ShapeDtypeStruct(shape, kind) if INTERPRET else pltpu.VMEM(shape, kind)


def call(kernel, args, specs, outs, out_specs, scratch=(), flops=0, traffic=0, mib=16, **more):
    return pl.pallas_call(
        kernel,
        in_specs=specs,
        out_specs=out_specs,
        out_shape=outs,
        scratch_shapes=list(scratch),
        interpret=INTERPRET,
        compiler_params=pltpu.CompilerParams(vmem_limit_bytes=mib << 20),
        cost_estimate=pl.CostEstimate(flops=flops, bytes_accessed=traffic, transcendentals=0),
        **more,
    )(*args)


def load_kernel(source, out, sem):
    copy = pltpu.make_async_copy(source, out, sem)
    copy.start()
    copy.wait()


def loaded(array):
    return call(
        load_kernel,
        [far(array)],
        [FAR],
        near_out(array.shape, array.dtype),
        CHIP,
        [pltpu.SemaphoreType.DMA],
        flops=array.size * 400,
        traffic=array.size * 4,
        mib=1,
    )


def quarters(turn, quarter):
    first = slice(turn * quarter, (turn + 1) * quarter)
    second = slice((1 - turn) * quarter, (2 - turn) * quarter)
    return first, second


def lay_out(place, offset, sides, lhs):
    half = lhs.shape[0] // len(sides)
    latent = sides[0][0].shape[2]
    for i, (turn, x) in enumerate(ORDER):
        rows_a, rows_b = quarters(turn, half // 2)
        for yh in range(2):
            layer = 2 * pair_of(place, offset, turn, x) + yh
            at = 4 * x + 2 * yh
            lanes = slice((2 * i + yh) * latent, (2 * i + yh + 1) * latent)

            @pl.when(layer <= place[1])
            def _():
                for side, (a, b) in enumerate(sides):
                    block = lhs.at[side * half : (side + 1) * half]
                    block[rows_a, lanes] = a[at + turn]
                    block[rows_b, lanes] = b[at + 1 - turn]

            @pl.when(layer > place[1])
            def _():
                lhs[:, lanes] = jnp.zeros((lhs.shape[0], latent), lhs.dtype)


def forward_kernel(offset, last, tokens, place, a, b, w, v, *rest):
    half = 2 * a.shape[1]
    columns = w.shape[2]
    if last:
        before, outputs, other, signal, signal_other, squares, lhs, wanted, wanted_other, sems = rest
        rows = pl.ds(pl.multiple_of(place[2] * half, 16), half)
        copy = pltpu.make_async_copy(outputs.at[rows, :], wanted, sems.at[0])
        copy.start()
        copy_other = pltpu.make_async_copy(other, wanted_other, sems.at[1])
        copy_other.start()
    else:
        total, lhs = rest
    lay_out(place, offset, [(a, b)], lhs)
    step = min(512, columns)
    pairs = [pair_of(place, offset, turn, x) for turn, x in ORDER]
    carry = jnp.zeros((16, 128), f32)
    for side, source in enumerate((w, v)):
        if last and side == 0:
            target, out = wanted, signal
        elif last:
            target, out = wanted_other, signal_other
        for start in range(0, columns, step):
            cols = slice(start, start + step)
            both = slice(side * columns + start, side * columns + start + step)
            rhs = jnp.concatenate([source[pair, :, cols] for pair in pairs], axis=0)
            product = jnp.dot(lhs[...], rhs, preferred_element_type=f32)
            if not last:
                total[:, both] = product
                continue
            if side == 0 and start == 0:
                copy.wait()
                copy_other.wait()
            misfit = product + before[:, both] - target[:, cols].astype(f32)
            out[:, cols] = (misfit * (1.0 / tokens)).astype(bf16)
            square = misfit * misfit
            square = jnp.sum(square.reshape(-1, 16, step), axis=0)
            for lane in range(0, step, 128):
                carry = carry + square[:, lane : lane + 128]
    if last:
        squares[...] = carry


def forward(offset, place, a, b, w, v, extra=None, tokens=None):
    quarter, latent = a.shape[1:]
    half = 2 * quarter
    depth, columns = w.shape[1:]
    last = extra is not None
    args = [place] + [near(t) for t in (a, b, w, v)]
    specs = [SCALARS] + [CHIP] * 4
    scratch = [pltpu.VMEM((half, 16 * latent), bf16)]
    if last:
        before, outputs, wanted_other = extra
        args += [near(before), far(outputs), far(wanted_other)]
        specs += [CHIP, FAR, FAR]
        outs = (near_out((half, columns), bf16), near_out((half, columns), bf16), near_out((16, 128), f32))
        out_specs = (CHIP,) * 3
        scratch += [pltpu.VMEM((half, columns), bf16)] * 2 + [pltpu.SemaphoreType.DMA((2,))]
    else:
        outs, out_specs = near_out((half, 2 * columns), f32), CHIP
    flops = 2 * half * 2 * columns * 8 * depth
    kernel = functools.partial(forward_kernel, offset, last, tokens)
    return call(kernel, args, specs, outs, out_specs, scratch, flops, 1 << 20)


def terms_kernel(offset, place, signal, signal_other, w, v, squares, fired, a, b):
    quarter, latent = a.shape[1] - EXTRA, a.shape[2]
    contract = (((1,), (1,)), ((), ()))
    loss = 0.5 * jnp.sum(squares[...]) + sparsity * jnp.sum(fired[...])
    loss = jnp.full((8, latent), loss, f32)
    high = loss.astype(bf16).astype(f32)
    note = jnp.concatenate([high, loss - high], axis=0).astype(bf16)
    for tile in range(a.shape[0]):
        a[tile, quarter:, :] = note
        b[tile, quarter:, :] = note
    for turn in range(2):
        pairs = [pair_of(place, offset, turn, x) for x in range(RING)]
        rows_a, rows_b = quarters(turn, quarter)
        term = None
        for left, right in ((signal, w), (signal_other, v)):
            rhs = jnp.concatenate([right[pair] for pair in pairs], axis=0)
            part = lax.dot_general(left[...], rhs, contract, preferred_element_type=f32)
            term = part if term is None else term + part
        term = term.astype(bf16)
        for x, yh in itertools.product(range(RING), range(2)):
            at = 4 * x + 2 * yh
            lanes = slice((2 * x + yh) * latent, (2 * x + yh + 1) * latent)
            kept = jnp.where(2 * pairs[x] + yh <= place[1], term[:, lanes], jnp.zeros((), bf16))
            a[at + turn, :quarter, :] = kept[rows_a]
            b[at + 1 - turn, :quarter, :] = kept[rows_b]


def terms_for(offset, place, signal, signal_other, w, v, squares, fired):
    half, columns = signal.shape
    depth = w.shape[1]
    latent = depth // 2
    args = [place] + [near(t) for t in (signal, signal_other, w, v, squares, fired)]
    out = near_out((16, half // 2 + EXTRA, latent), bf16)
    flops = 2 * half * 2 * columns * 8 * depth
    kernel = functools.partial(terms_kernel, offset)
    return call(kernel, args, [SCALARS] + [CHIP] * 6, (out, out), (CHIP, CHIP), (), flops, 1 << 20)


def gradient_kernel(offset, place, a, b, a_other, b_other, signal, signal_other, *rest):
    out, lhs, rhs, held, sems = rest[-5:]
    half = signal.shape[0]
    depth = held.shape[1]
    rhs[:half, :] = signal[...]
    rhs[half:, :] = signal_other[...]
    lay_out(place, offset, [(a, b), (a_other, b_other)], lhs)
    contract = (((0,), (0,)), ((), ()))
    copies = []
    for i in range(0, len(ORDER), 2):
        left = lhs[:, i * depth : (i + 2) * depth]
        product = lax.dot_general(left, rhs[...], contract, preferred_element_type=f32).astype(bf16)
        for j in range(2):
            held[i + j] = product[j * depth : (j + 1) * depth]
            pair = pair_of(place, offset, *ORDER[i + j])
            copy = pltpu.make_async_copy(held.at[i + j], out.at[pair], sems.at[i + j])
            copy.start()
            copies.append(copy)
    for copy in copies:
        copy.wait()


def gradient(offset, place, a, b, a_other, b_other, signal, signal_other, so_far=None):
    latent = a.shape[2]
    half, columns = signal.shape
    args = [place] + [near(t) for t in (a, b, a_other, b_other)] + [signal, signal_other]
    specs = [SCALARS] + [CHIP] * 6
    aliases = {}
    if so_far is not None:
        aliases = {len(args): 0}
        args.append(so_far)
        specs.append(FAR)
    scratch = [
        pltpu.VMEM((2 * half, 16 * latent), bf16),
        pltpu.VMEM((2 * half, columns), bf16),
        pltpu.VMEM((len(ORDER), 2 * latent, columns), bf16),
        pltpu.SemaphoreType.DMA((len(ORDER),)),
    ]
    out = jax.ShapeDtypeStruct((RING * RING, 2 * latent, columns), bf16)
    flops = 2 * 2 * half * columns * 16 * latent
    kernel = functools.partial(gradient_kernel, offset)
    return call(kernel, args, specs, out, FAR, scratch, flops, 1 << 20, mib=20, input_output_aliases=aliases)


def sum_kernel(own, one, two, three, out):
    quarter = own.shape[1] - EXTRA
    parts = (own, one, two, three)
    for tile in range(own.shape[0]):
        total = functools.reduce(lambda s, p: s + p, [p[tile, :quarter, :].astype(f32) for p in parts])
        out[tile, :quarter, :] = total.astype(bf16)
        row = lax.broadcasted_iota(jnp.int32, (EXTRA, own.shape[2]), 0)
        note = jnp.zeros((EXTRA, own.shape[2]), f32)
        for i, part in enumerate(parts):
            heard = part[tile, quarter:, :].astype(f32)
            high = jnp.broadcast_to(heard[:1], heard.shape)
            low = jnp.broadcast_to(heard[8:9], heard.shape)
            note = jnp.where(row == 2 * i, high, jnp.where(row == 2 * i + 1, low, note))
        out[tile, quarter:, :] = note.astype(bf16)


def summed(*parts):
    args = [near(part) for part in parts]
    out = jax.ShapeDtypeStruct(parts[0].shape, bf16)
    return call(sum_kernel, args, [CHIP] * 4, out, CHIP, (), 1 << 20, 1 << 20, mib=4)


def delta_kernel(tokens, arrived, potential, delta, loss):
    quarter = potential.shape[0]
    total = arrived[0, :quarter, :].astype(f32)
    for tile in range(1, arrived.shape[0]):
        total = total + arrived[tile, :quarter, :].astype(f32)
    total = jnp.where(potential[...] > 0, total + sparsity / tokens, 0.0)
    delta[...] = total.astype(bf16)
    losses = []
    for tile in range(arrived.shape[0]):
        notes = arrived[tile, quarter:, :].astype(f32)
        losses += [notes[2 * i : 2 * i + 1] + notes[2 * i + 1 : 2 * i + 2] for i in range(RING)]
    unit = jnp.maximum(functools.reduce(jnp.maximum, losses), 1e-30)
    whole = functools.reduce(lambda p, q: p + q, [jnp.round(value / unit * 65536.0) for value in losses])
    loss[...] = jnp.broadcast_to(whole * (unit / 65536.0), loss.shape)


def delta_of(arrived, potential, tokens):
    quarter, latent = potential.shape
    args = [near(arrived), potential]
    outs = (near_out((quarter, latent), bf16), near_out((8, latent), f32))
    kernel = functools.partial(delta_kernel, tokens)
    return call(kernel, args, [CHIP] * 2, outs, (CHIP, CHIP), (), 1 << 20, 1 << 20, mib=8)


def finish_kernel(size, place, inputs, own, beside, opposite, last, loss, loss_other, encoder, bias, mean, delta):
    quarter = own.shape[0]
    core, side = place[2], place[3]
    parts = ((own, core, side), (beside, core, 1 - side), (opposite, 1 - core, side), (last, 1 - core, 1 - side))
    for part, c, y in parts:
        delta[pl.ds(pl.multiple_of((2 * c + y) * quarter, 16), quarter), :] = part[...]
    contract = (((0,), (0,)), ((), ()))
    product = lax.dot_general(inputs[...], delta[...], contract, preferred_element_type=f32)
    encoder[...] = product.astype(bf16)
    bias[...] = jnp.sum(delta[...].astype(f32), axis=0, keepdims=True)
    mean[0, 0] = (jnp.max(loss[...]) + jnp.max(loss_other[...])) / size


def finished(size, place, inputs, *parts):
    tokens, columns = inputs.shape
    latent = parts[0].shape[1]
    args = [place] + [near(t) for t in (inputs, *parts)]
    outs = (
        jax.ShapeDtypeStruct((columns, latent), bf16),
        jax.ShapeDtypeStruct((1, latent), f32),
        jax.ShapeDtypeStruct((1, 1), f32),
    )
    scratch = [pltpu.VMEM((tokens, latent), bf16)]
    kernel = functools.partial(finish_kernel, size)
    return call(kernel, args, [SCALARS] + [CHIP] * 7, outs, (CHIP, CHIP, SCALARS), scratch, 1 << 20, 1 << 20, mib=8)


def whole_step(mlp_inputs, mlp_outputs, encoders, encoder_bias, decoders):
    inputs = mlp_inputs[0]
    tokens = inputs.shape[0]
    width = inputs.shape[1] * lax.axis_size(WIDTH)
    layers = lax.axis_size(LAYER)
    latent = encoders.shape[2]
    own_layer = lax.axis_index(LAYER)
    core, side = lax.axis_index("c"), lax.axis_index("yl")
    coset = lax.rem(lax.axis_index("x") + lax.axis_index("z") + 2 * side, RING)
    place = jnp.stack([coset, own_layer, core, side]).astype(jnp.int32)

    partial = jnp.dot(inputs, encoders[0], preferred_element_type=f32)
    mine, theirs = halves(partial, "c")
    heard = swapped(theirs, "c")
    weights = decoders[0].reshape(layers // 2, 2 * latent, -1)
    outputs = mlp_outputs[0]
    heard, weights, outputs = lax.optimization_barrier((heard, weights, outputs))
    partial = mine + heard
    weights_other = swapped(weights, "c")
    mine, theirs = halves(partial, "yl")
    heard = swapped(theirs, "yl")
    potential = mine + heard + encoder_bias[0][None, :]
    active = jnp.maximum(potential, 0.0)
    firing = active.astype(bf16)
    fired = jnp.sum(active.reshape(-1, 8, latent), axis=0)

    own = in_coset(jnp.broadcast_to(firing[None], (16, *firing.shape)))
    two = sent(own, 2)
    one = sent(own, 1)
    three = sent(own, 3)
    own_other = swapped(own, "c")
    two_other = swapped(two, "c")
    one_other = swapped(one, "c")
    three_other = swapped(three, "c")
    own, outputs = lax.optimization_barrier((own, outputs))
    half = tokens // 2
    wanted_sent = lax.dynamic_slice_in_dim(outputs, (1 - core) * half, half, 0)
    wanted_other = swapped(wanted_sent, "c")

    weights = loaded(weights)
    weights_other = loaded(weights_other)
    total = forward(0, place, own, two, weights, weights_other)
    signal, signal_other, squares = forward(
        1, place, three, one, weights, weights_other, (total, outputs, wanted_other), tokens
    )
    signal_here = swapped(signal_other, "c")

    rest = (place, signal, signal_other, weights, weights_other, squares, fired)
    to_three, to_one = terms_for(1, *rest)
    from_one = sent(to_one, 1, back=True)
    from_three = sent(to_three, 3, back=True)
    at_home, to_two = terms_for(0, *rest)
    from_two = sent(to_two, 2, back=True)
    signals = (signal, signal_here)
    grad_decoder = gradient(0, place, own, two, own_other, two_other, *signals)
    arrived = in_coset(summed(at_home, from_one, from_two, from_three))
    grad_decoder = gradient(1, place, three, one, three_other, one_other, *signals, grad_decoder)

    delta, loss = delta_of(arrived, potential, tokens)
    opposite = swapped(delta, "c")
    beside = swapped(delta, "yl")
    loss_other = swapped(loss, "c")
    last = swapped(beside, "c")
    size = float(tokens * width * layers)
    grad_encoder, grad_bias, loss_mean = finished(
        size, place, inputs, delta, beside, opposite, last, loss, loss_other
    )
    return (loss_mean[0, 0], grad_encoder[None], grad_bias, grad_decoder.reshape(decoders.shape))


def solution(mesh):
    finer = Mesh(mesh.devices.reshape(4, 4, 2, 2, 2), AXES)
    placed = (
        P(LAYER, None, WIDTH),
        P(LAYER, None, WIDTH),
        P(LAYER, WIDTH, None),
        P(LAYER, None),
        P(LAYER, None, None, WIDTH),
    )
    return jax.shard_map(
        whole_step,
        mesh=finer,
        in_specs=placed,
        out_specs=(P(), P(LAYER, WIDTH, None), P(LAYER, None), P(LAYER, None, None, WIDTH)),
        check_vma=False,
    )
```

```python
import functools
import itertools

import jax
import jax.numpy as jnp
from jax import lax
from jax.experimental import pallas as pl
from jax.experimental.pallas import tpu as pltpu
from jax.sharding import Mesh
from jax.sharding import PartitionSpec as P

AXES = ("x", "z", "yh", "yl", "c")
LAYER = ("x", "z", "yh")
WIDTH = ("yl", "c")
SWAP = [(0, 1), (1, 0)]
RING = 4
EXTRA = 16
INTERPRET = False

sparsity = 8.0
f32, bf16 = jnp.float32, jnp.bfloat16


def flat(x, z, y, c):
    return ((x % RING * RING + z % RING) * RING + y % RING) * 2 + c


def toward(shift, back=False):
    pairs = []
    for x, z, y, c in itertools.product(range(RING), range(RING), range(RING), range(2)):
        if c == 0:
            there = {1: (x + 1, z, y), 3: (x - 1, z, y), 2: (x, z, y + 1)}[shift]
        else:
            there = {1: (x, z + 1, y), 3: (x, z - 1, y), 2: (x, z, y - 1)}[shift]
        pair = (flat(x, z, y, c), flat(*there, c))
        pairs.append(pair[::-1] if back else pair)
    return pairs


COSETS = [
    [flat(x, f - x - 2 * yl, 2 * yh + yl, c) for x in range(RING) for yh in range(2) for yl in range(2)]
    for f in range(RING)
    for c in range(2)
]


def sent(array, shift, back=False):
    return lax.ppermute(array, AXES, toward(shift, back))


def in_coset(blocks):
    return lax.all_to_all(blocks, AXES, 0, 0, axis_index_groups=COSETS, tiled=True)


def swapped(array, axis):
    return lax.ppermute(array, axis, SWAP)


def halves(array, axis, dim=0):
    half = array.shape[dim] // 2
    own = lax.axis_index(axis)
    mine = lax.dynamic_slice_in_dim(array, own * half, half, dim)
    theirs = lax.dynamic_slice_in_dim(array, (1 - own) * half, half, dim)
    return mine, theirs


def placement():
    x, side = lax.axis_index("x"), lax.axis_index("yl")
    coset = lax.rem(x + lax.axis_index("z") + 2 * side, RING)
    tile = 4 * x + 2 * lax.axis_index("yh") + side
    return coset, lax.axis_index(LAYER), lax.axis_index("c"), side, tile


def pair_of(place, offset, turn, x):
    return RING * x + lax.rem(place[0] + offset + 2 * turn + RING - x, RING)


ORDER = tuple(itertools.product(range(2), range(RING)))
CHIP = pl.BlockSpec(memory_space=pltpu.VMEM)
SCALARS = pl.BlockSpec(memory_space=pltpu.SMEM)
FAR = pl.BlockSpec(memory_space=pltpu.HBM)
ANY = pl.BlockSpec(memory_space=pl.ANY)


def near(array):
    return array if INTERPRET else pltpu.with_memory_space_constraint(array, pltpu.VMEM)


def far(array):
    return array if INTERPRET else pltpu.with_memory_space_constraint(array, pltpu.HBM)


def near_out(shape, kind):
    return jax.ShapeDtypeStruct(shape, kind) if INTERPRET else pltpu.VMEM(shape, kind)


def call(kernel, args, specs, outs, out_specs, scratch=(), flops=0, traffic=0, mib=16, **more):
    return pl.pallas_call(
        kernel,
        in_specs=specs,
        out_specs=out_specs,
        out_shape=outs,
        scratch_shapes=list(scratch),
        interpret=INTERPRET,
        compiler_params=pltpu.CompilerParams(vmem_limit_bytes=mib << 20),
        cost_estimate=pl.CostEstimate(flops=flops, bytes_accessed=traffic, transcendentals=0),
        **more,
    )(*args)


def load_kernel(source, out, sem):
    place = placement()
    depth = source.shape[1] // 2
    for pair, yh in itertools.product(range(source.shape[0]), range(2)):
        rows = slice(yh * depth, (yh + 1) * depth)
        used = 2 * pair + yh <= place[1]

        @pl.when(used)
        def _():
            pltpu.make_async_copy(source.at[pair, rows, :], out.at[pair, rows, :], sem.at[pair, yh]).start()

        @pl.when(jnp.logical_not(used))
        def _():
            out[pair, rows, :] = jnp.zeros((depth, source.shape[2]), out.dtype)

    for pair, yh in itertools.product(range(source.shape[0]), range(2)):
        rows = slice(yh * depth, (yh + 1) * depth)

        @pl.when(2 * pair + yh <= place[1])
        def _():
            pltpu.make_async_copy(source.at[pair, rows, :], out.at[pair, rows, :], sem.at[pair, yh]).wait()


def loaded(array):
    return call(
        load_kernel,
        [far(array)],
        [FAR],
        near_out(array.shape, array.dtype),
        CHIP,
        [pltpu.SemaphoreType.DMA((array.shape[0], 2))],
        flops=array.size * 400,
        traffic=array.size * 4,
        mib=1,
    )


def quarters(turn, quarter):
    first = slice(turn * quarter, (turn + 1) * quarter)
    second = slice((1 - turn) * quarter, (2 - turn) * quarter)
    return first, second


def lay_out_pair(a, b, lhs):
    quarter, latent = a.shape[1:]
    for i, (turn, x) in enumerate(ORDER):
        rows_a, rows_b = quarters(turn, quarter)
        for yh in range(2):
            at = 4 * x + 2 * yh
            lanes = slice((2 * i + yh) * latent, (2 * i + yh + 1) * latent)
            lhs[rows_a, lanes] = a[at + turn]
            lhs[rows_b, lanes] = b[at + 1 - turn]


def lay_out(place, offset, sides, lhs):
    half = lhs.shape[0] // len(sides)
    latent = sides[0][0].shape[2]
    for i, (turn, x) in enumerate(ORDER):
        rows_a, rows_b = quarters(turn, half // 2)
        for yh in range(2):
            layer = 2 * pair_of(place, offset, turn, x) + yh
            at = 4 * x + 2 * yh
            lanes = slice((2 * i + yh) * latent, (2 * i + yh + 1) * latent)

            @pl.when(layer <= place[1])
            def _():
                for side, (a, b) in enumerate(sides):
                    block = lhs.at[side * half : (side + 1) * half]
                    block[rows_a, lanes] = a[at + turn]
                    block[rows_b, lanes] = b[at + 1 - turn]

            @pl.when(layer > place[1])
            def _():
                lhs[:, lanes] = jnp.zeros((lhs.shape[0], latent), lhs.dtype)


def lay_out_block(block, lhs):
    quarter, latent = block.shape[1:]
    for q, x, yh in itertools.product(range(2), range(RING), range(2)):
        rows = slice(q * quarter, (q + 1) * quarter)
        lanes = slice((2 * x + yh) * latent, (2 * x + yh + 1) * latent)
        lhs[rows, lanes] = block[4 * x + 2 * yh + q]


def block_product(place, shift, lhs, source, cols):
    quarter = lhs.shape[0] // 2
    parts = []
    for q in range(2):
        pairs = [pair_of(place, shift, q, x) for x in range(RING)]
        rhs = jnp.concatenate([source[pair, :, cols] for pair in pairs], axis=0)
        rows = slice(q * quarter, (q + 1) * quarter)
        parts.append(jnp.dot(lhs[rows, :], rhs, preferred_element_type=f32))
    return jnp.concatenate(parts, axis=0)


def column_steps(columns):
    step = min(512, columns)
    for start in range(0, columns, step):
        yield start, slice(start, start + step)


def home_kernel(block, w, v, total, lhs):
    place = placement()
    lay_out_block(block, lhs)
    columns = w.shape[2]
    for side, source in enumerate((w, v)):
        for start, cols in column_steps(columns):
            both = slice(side * columns + start, side * columns + cols.stop)
            total[:, both] = block_product(place, 0, lhs, source, cols)


def rebuilt_home(block, w, v):
    quarter, latent = block.shape[1:]
    half = 2 * quarter
    depth, columns = w.shape[1:]
    args = [near(t) for t in (block, w, v)]
    scratch = [pltpu.VMEM((half, 8 * latent), bf16)]
    out = near_out((half, 2 * columns), f32)
    flops = half * 2 * columns * 8 * depth
    return call(home_kernel, args, [CHIP] * 3, out, CHIP, scratch, flops, 1 << 20)


def forward_kernel(tokens, two, a, b, w, v, before, outputs, other, *rest):
    place = placement()
    signal, signal_other, squares, lhs, lhs_two, wanted, wanted_other, sems = rest
    half = 2 * a.shape[1]
    columns = w.shape[2]
    rows = pl.ds(pl.multiple_of(place[2] * half, 16), half)
    copy = pltpu.make_async_copy(outputs.at[rows, :], wanted, sems.at[0])
    copy.start()
    copy_other = pltpu.make_async_copy(other, wanted_other, sems.at[1])
    copy_other.start()
    lay_out_block(two, lhs_two)
    lay_out_pair(a, b, lhs)
    pairs = [pair_of(place, 1, turn, x) for turn, x in ORDER]
    carry = jnp.zeros((16, 128), f32)
    sides = ((w, wanted, signal), (v, wanted_other, signal_other))
    for side, (source, target, out) in enumerate(sides):
        for start, cols in column_steps(columns):
            both = slice(side * columns + start, side * columns + cols.stop)
            rhs = jnp.concatenate([source[pair, :, cols] for pair in pairs], axis=0)
            product = jnp.dot(lhs[...], rhs, preferred_element_type=f32)
            product = product + block_product(place, 2, lhs_two, source, cols)
            if side == 0 and start == 0:
                copy.wait()
                copy_other.wait()
            misfit = product + before[:, both] - target[:, cols].astype(f32)
            out[:, cols] = (misfit * (1.0 / tokens)).astype(bf16)
            square = misfit * misfit
            square = jnp.sum(square.reshape(-1, 16, square.shape[1]), axis=0)
            for lane in range(0, square.shape[1], 128):
                carry = carry + square[:, lane : lane + 128]
    squares[...] = carry


def forward(tokens, two, a, b, w, v, before, outputs, wanted_other):
    quarter, latent = a.shape[1:]
    half = 2 * quarter
    depth, columns = w.shape[1:]
    args = [near(t) for t in (two, a, b, w, v, before)] + [far(outputs), wanted_other]
    specs = [CHIP] * 6 + [FAR, ANY]
    scratch = [pltpu.VMEM((half, 16 * latent), bf16), pltpu.VMEM((half, 8 * latent), bf16)]
    scratch += [pltpu.VMEM((half, columns), bf16)] * 2 + [pltpu.SemaphoreType.DMA((2,))]
    outs = (near_out((half, columns), bf16), near_out((half, columns), bf16), near_out((16, 128), f32))
    flops = 3 * half * 2 * columns * 8 * depth
    kernel = functools.partial(forward_kernel, tokens)
    return call(kernel, args, specs, outs, (CHIP,) * 3, scratch, flops, 1 << 20)


def write_notes(squares, fired, *blocks):
    quarter, latent = blocks[0].shape[1] - EXTRA, blocks[0].shape[2]
    loss = 0.5 * jnp.sum(squares[...]) + sparsity * jnp.sum(fired[...])
    loss = jnp.full((8, latent), loss, f32)
    high = loss.astype(bf16).astype(f32)
    note = jnp.concatenate([high, loss - high], axis=0).astype(bf16)
    for block in blocks:
        for tile in range(block.shape[0]):
            block[tile, quarter:, :] = note


NT = (((1,), (1,)), ((), ()))


def terms_kernel(offset, signal, signal_other, w, v, squares, fired, a, b):
    place = placement()
    quarter, latent = a.shape[1] - EXTRA, a.shape[2]
    write_notes(squares, fired, a, b)
    for turn in range(2):
        pairs = [pair_of(place, offset, turn, x) for x in range(RING)]
        rows_a, rows_b = quarters(turn, quarter)
        term = None
        for left, right in ((signal, w), (signal_other, v)):
            rhs = jnp.concatenate([right[pair] for pair in pairs], axis=0)
            part = lax.dot_general(left[...], rhs, NT, preferred_element_type=f32)
            term = part if term is None else term + part
        term = term.astype(bf16)
        for x, yh in itertools.product(range(RING), range(2)):
            at = 4 * x + 2 * yh
            lanes = slice((2 * x + yh) * latent, (2 * x + yh + 1) * latent)
            a[at + turn, :quarter, :] = term[rows_a, lanes]
            b[at + 1 - turn, :quarter, :] = term[rows_b, lanes]


def terms_for(offset, signal, signal_other, w, v, squares, fired):
    half, columns = signal.shape
    depth = w.shape[1]
    latent = depth // 2
    args = [near(t) for t in (signal, signal_other, w, v, squares, fired)]
    out = near_out((16, half // 2 + EXTRA, latent), bf16)
    flops = 2 * half * 2 * columns * 8 * depth
    kernel = functools.partial(terms_kernel, offset)
    return call(kernel, args, [CHIP] * 6, (out, out), (CHIP, CHIP), (), flops, 1 << 20)


def gradient_kernel(offset, a, b, a_other, b_other, signal, signal_other, *rest):
    place = placement()
    out, lhs, rhs, held, sems, sems_in = rest[-6:]
    half = signal.shape[0]
    depth = held.shape[1]
    incoming = pltpu.make_async_copy(signal, rhs.at[:half, :], sems_in.at[0])
    incoming.start()
    incoming_other = pltpu.make_async_copy(signal_other, rhs.at[half:, :], sems_in.at[1])
    incoming_other.start()
    lay_out(place, offset, [(a, b), (a_other, b_other)], lhs)
    incoming.wait()
    incoming_other.wait()
    contract = (((0,), (0,)), ((), ()))
    copies = []
    for i in range(0, len(ORDER), 2):
        left = lhs[:, i * depth : (i + 2) * depth]
        product = lax.dot_general(left, rhs[...], contract, preferred_element_type=f32).astype(bf16)
        for j in range(2):
            held[i + j] = product[j * depth : (j + 1) * depth]
            pair = pair_of(place, offset, *ORDER[i + j])
            copy = pltpu.make_async_copy(held.at[i + j], out.at[pair], sems.at[i + j])
            copy.start()
            copies.append(copy)
    for copy in copies:
        copy.wait()


def gradient(offset, a, b, a_other, b_other, signal, signal_other, so_far=None):
    latent = a.shape[2]
    half, columns = signal.shape
    args = [near(t) for t in (a, b, a_other, b_other)] + [signal, far(signal_other)]
    specs = [CHIP] * 4 + [ANY, FAR]
    aliases = {}
    if so_far is not None:
        aliases = {len(args): 0}
        args.append(so_far)
        specs.append(FAR)
    scratch = [
        pltpu.VMEM((2 * half, 16 * latent), bf16),
        pltpu.VMEM((2 * half, columns), bf16),
        pltpu.VMEM((len(ORDER), 2 * latent, columns), bf16),
        pltpu.SemaphoreType.DMA((len(ORDER),)),
        pltpu.SemaphoreType.DMA((2,)),
    ]
    out = jax.ShapeDtypeStruct((RING * RING, 2 * latent, columns), bf16)
    flops = 2 * 2 * half * columns * 16 * latent
    kernel = functools.partial(gradient_kernel, offset)
    return call(kernel, args, specs, out, FAR, scratch, flops, 1 << 20, mib=20, input_output_aliases=aliases)


def sum_kernel(own, one, two, three, out):
    quarter = own.shape[1] - EXTRA
    parts = (own, one, two, three)
    for tile in range(own.shape[0]):
        total = functools.reduce(lambda s, p: s + p, [p[tile, :quarter, :].astype(f32) for p in parts])
        out[tile, :quarter, :] = total.astype(bf16)
        row = lax.broadcasted_iota(jnp.int32, (EXTRA, own.shape[2]), 0)
        note = jnp.zeros((EXTRA, own.shape[2]), f32)
        for i, part in enumerate(parts):
            heard = part[tile, quarter:, :].astype(f32)
            high = jnp.broadcast_to(heard[:1], heard.shape)
            low = jnp.broadcast_to(heard[8:9], heard.shape)
            note = jnp.where(row == 2 * i, high, jnp.where(row == 2 * i + 1, low, note))
        out[tile, quarter:, :] = note.astype(bf16)


def summed(*parts):
    args = [near(part) for part in parts]
    out = jax.ShapeDtypeStruct(parts[0].shape, bf16)
    return call(sum_kernel, args, [CHIP] * 4, out, CHIP, (), 1 << 20, 1 << 20, mib=4)


def encode_kernel(flip, inputs, weights, *rest):
    place = placement()
    out, rows_here, weights_here, sems = rest[-4:]
    half = out.shape[0]
    which = 1 - place[2] if flip else place[2]
    rows = pl.ds(pl.multiple_of(which * half, 16), half)
    copies = (
        pltpu.make_async_copy(inputs.at[rows, :], rows_here, sems.at[0]),
        pltpu.make_async_copy(weights, weights_here, sems.at[1]),
    )
    for copy in copies:
        copy.start()
    for copy in copies:
        copy.wait()
    out[...] = jnp.dot(rows_here[...], weights_here[...], preferred_element_type=f32)
    if not flip:

        @pl.when(place[3] == 0)
        def _():
            out[...] += rest[0][...]


def encoded(flip, inputs, weights, bias):
    tokens, columns = inputs.shape
    latent = weights.shape[1]
    scratch = [
        pltpu.VMEM((tokens // 2, columns), bf16),
        pltpu.VMEM((columns, latent), bf16),
        pltpu.SemaphoreType.DMA((2,)),
    ]
    out = near_out((tokens // 2, latent), f32)
    kernel = functools.partial(encode_kernel, flip)
    args = [far(inputs), far(weights)] + ([] if flip else [bias])
    return call(kernel, args, [FAR, FAR, CHIP][: len(args)], out, CHIP, scratch, 1 << 20, 1 << 20, mib=4)


def fire_kernel(mine, heard, fired, blocks):
    place = placement()
    quarter = heard.shape[0]
    rows = pl.ds(pl.multiple_of(place[3] * quarter, 16), quarter)
    value = mine[rows, :] + heard[...]
    active = jnp.maximum(value, 0.0)
    fired[...] = jnp.sum(active.reshape(-1, 8, active.shape[1]), axis=0)
    firing = active.astype(bf16)
    for tile in range(blocks.shape[0]):
        blocks[tile] = firing


def fire(mine, heard):
    quarter, latent = heard.shape
    args = [near(mine), near(heard)]
    outs = (
        near_out((8, latent), f32),
        near_out((16, quarter, latent), bf16),
    )
    return call(fire_kernel, args, [CHIP] * 2, outs, (CHIP,) * 2, (), 1 << 20, 1 << 20, mib=4)


def delta_kernel(tokens, arrived, firing, delta):
    place = placement()
    quarter, latent = firing.shape[1:]
    total = arrived[0, :quarter, :].astype(f32)
    for tile in range(1, arrived.shape[0]):
        total = total + arrived[tile, :quarter, :].astype(f32)
    positive = firing[place[4]].astype(f32) > 0
    total = jnp.where(positive, total + sparsity / tokens, 0.0)
    delta[:quarter, :] = total.astype(bf16)
    losses = []
    for tile in range(arrived.shape[0]):
        notes = arrived[tile, quarter:, :].astype(f32)
        losses += [notes[2 * i : 2 * i + 1] + notes[2 * i + 1 : 2 * i + 2] for i in range(RING)]
    unit = jnp.maximum(functools.reduce(jnp.maximum, losses), 1e-30)
    whole = functools.reduce(lambda p, q: p + q, [jnp.round(value / unit * 65536.0) for value in losses])
    loss = jnp.broadcast_to(whole * (unit / 65536.0), (8, latent))
    high = loss.astype(bf16).astype(f32)
    delta[quarter:, :] = jnp.concatenate([high, loss - high], axis=0).astype(bf16)


def delta_of(arrived, firing, tokens):
    quarter, latent = firing.shape[1:]
    args = [near(arrived), near(firing)]
    out = near_out((quarter + EXTRA, latent), bf16)
    kernel = functools.partial(delta_kernel, tokens)
    return call(kernel, args, [CHIP] * 2, out, CHIP, (), 1 << 20, 1 << 20, mib=8)


def finish_kernel(size, inputs, own, beside, opposite, last, encoder, bias, mean, delta):
    place = placement()
    quarter = own.shape[0] - EXTRA
    core, side = place[2], place[3]
    parts = ((own, core, side), (beside, core, 1 - side), (opposite, 1 - core, side), (last, 1 - core, 1 - side))
    for part, c, y in parts:
        delta[pl.ds(pl.multiple_of((2 * c + y) * quarter, 16), quarter), :] = part[:quarter, :]
    contract = (((0,), (0,)), ((), ()))
    product = lax.dot_general(inputs[...], delta[...], contract, preferred_element_type=f32)
    encoder[...] = product.astype(bf16)
    bias[...] = jnp.sum(delta[...].astype(f32), axis=0, keepdims=True)
    losses = []
    for part in (own, opposite):
        notes = part[quarter:, :].astype(f32)
        losses.append(jnp.max(notes[:8] + notes[8:]))
    mean[0, 0] = (losses[0] + losses[1]) / size


def finished(size, inputs, *parts):
    tokens, columns = inputs.shape
    latent = parts[0].shape[1]
    args = [near(t) for t in (inputs, *parts)]
    outs = (
        jax.ShapeDtypeStruct((columns, latent), bf16),
        jax.ShapeDtypeStruct((1, latent), f32),
        jax.ShapeDtypeStruct((1, 1), f32),
    )
    scratch = [pltpu.VMEM((tokens, latent), bf16)]
    kernel = functools.partial(finish_kernel, size)
    return call(kernel, args, [CHIP] * 5, outs, (CHIP, CHIP, SCALARS), scratch, 1 << 20, 1 << 20, mib=8)


def whole_step(mlp_inputs, mlp_outputs, encoders, encoder_bias, decoders):
    inputs = mlp_inputs[0]
    tokens = inputs.shape[0]
    width = inputs.shape[1] * lax.axis_size(WIDTH)
    layers = lax.axis_size(LAYER)
    latent = encoders.shape[2]
    core = lax.axis_index("c")

    theirs = encoded(True, inputs, encoders[0], encoder_bias)
    heard = swapped(theirs, "c")
    mine = encoded(False, inputs, encoders[0], encoder_bias)
    weights = decoders[0].reshape(layers // 2, 2 * latent, -1)
    outputs = mlp_outputs[0]
    heard, weights, outputs = lax.optimization_barrier((heard, weights, outputs))
    partial = mine + heard
    weights_other = swapped(weights, "c")
    _, theirs = halves(partial, "yl")
    half = tokens // 2
    wanted_sent = lax.dynamic_slice_in_dim(outputs, (1 - core) * half, half, 0)
    wanted_other = swapped(wanted_sent, "c")
    heard = swapped(theirs, "yl")
    fired, blocks = fire(partial, heard)

    own = in_coset(blocks)
    two = sent(own, 2)
    one = sent(own, 1)
    three = sent(own, 3)
    own_other = swapped(own, "c")
    two_other = swapped(two, "c")
    one_other = swapped(one, "c")
    three_other = swapped(three, "c")

    weights = loaded(weights)
    weights_other = loaded(weights_other)
    total = rebuilt_home(own, weights, weights_other)
    signal, signal_other, squares = forward(
        tokens, two, three, one, weights, weights_other, total, outputs, wanted_other
    )
    signal_here = swapped(signal_other, "c")

    rest = (signal, signal_other, weights, weights_other, squares, fired)
    at_home, to_two = terms_for(0, *rest)
    from_two = sent(to_two, 2, back=True)
    to_three, to_one = terms_for(1, *rest)
    from_one = sent(to_one, 1, back=True)
    from_three = sent(to_three, 3, back=True)
    signals = (signal, signal_here)
    grad_decoder = gradient(0, own, two, own_other, two_other, *signals)
    arrived = in_coset(summed(at_home, from_one, from_two, from_three))
    grad_decoder = gradient(1, three, one, three_other, one_other, *signals, grad_decoder)

    delta = delta_of(arrived, own, tokens)
    beside = swapped(delta, "yl")
    last = lax.ppermute(delta, WIDTH, [(0, 3), (1, 2), (2, 1), (3, 0)])
    opposite = swapped(delta, "c")
    size = float(tokens * width * layers)
    grad_encoder, grad_bias, loss_mean = finished(
        size, inputs, delta, beside, opposite, last
    )
    return (loss_mean[0, 0], grad_encoder[None], grad_bias, grad_decoder.reshape(decoders.shape))


def solution(mesh):
    finer = Mesh(mesh.devices.reshape(4, 4, 2, 2, 2), AXES)
    placed = (
        P(LAYER, None, WIDTH),
        P(LAYER, None, WIDTH),
        P(LAYER, WIDTH, None),
        P(LAYER, None),
        P(LAYER, None, None, WIDTH),
    )
    return jax.shard_map(
        whole_step,
        mesh=finer,
        in_specs=placed,
        out_specs=(P(), P(LAYER, WIDTH, None), P(LAYER, None), P(LAYER, None, None, WIDTH)),
        check_vma=False,
    )
```

```python
import functools
import itertools

import jax
import jax.numpy as jnp
from jax import lax
from jax.experimental import pallas as pl
from jax.experimental.pallas import tpu as pltpu
from jax.sharding import Mesh
from jax.sharding import PartitionSpec as P

AXES = ("x", "z", "yh", "yl", "c")
LAYER = ("x", "z", "yh")
WIDTH = ("yl", "c")
SWAP = [(0, 1), (1, 0)]
RING = 4
EXTRA = 16
INTERPRET = False

sparsity = 8.0
f32, bf16 = jnp.float32, jnp.bfloat16


def flat(x, z, y, c):
    return ((x % RING * RING + z % RING) * RING + y % RING) * 2 + c


def toward(shift, back=False):
    pairs = []
    for x, z, y, c in itertools.product(range(RING), range(RING), range(RING), range(2)):
        if c == 0:
            there = {1: (x + 1, z, y), 3: (x - 1, z, y), 2: (x, z, y + 1)}[shift]
        else:
            there = {1: (x, z + 1, y), 3: (x, z - 1, y), 2: (x, z, y - 1)}[shift]
        pair = (flat(x, z, y, c), flat(*there, c))
        pairs.append(pair[::-1] if back else pair)
    return pairs


COSETS = [
    [flat(x, f - x - 2 * yl, 2 * yh + yl, c) for x in range(RING) for yh in range(2) for yl in range(2)]
    for f in range(RING)
    for c in range(2)
]


def sent(array, shift, back=False):
    return lax.ppermute(array, AXES, toward(shift, back))


def in_coset(blocks):
    return lax.all_to_all(blocks, AXES, 0, 0, axis_index_groups=COSETS, tiled=True)


def swapped(array, axis):
    return lax.ppermute(array, axis, SWAP)


def halves(array, axis, dim=0):
    half = array.shape[dim] // 2
    own = lax.axis_index(axis)
    mine = lax.dynamic_slice_in_dim(array, own * half, half, dim)
    theirs = lax.dynamic_slice_in_dim(array, (1 - own) * half, half, dim)
    return mine, theirs


def placement():
    x, side = lax.axis_index("x"), lax.axis_index("yl")
    coset = lax.rem(x + lax.axis_index("z") + 2 * side, RING)
    tile = 4 * x + 2 * lax.axis_index("yh") + side
    return coset, lax.axis_index(LAYER), lax.axis_index("c"), side, tile


def pair_of(place, offset, turn, x):
    return RING * x + lax.rem(place[0] + offset + 2 * turn + RING - x, RING)


ORDER = tuple(itertools.product(range(2), range(RING)))
CHIP = pl.BlockSpec(memory_space=pltpu.VMEM)
SCALARS = pl.BlockSpec(memory_space=pltpu.SMEM)
FAR = pl.BlockSpec(memory_space=pltpu.HBM)
ANY = pl.BlockSpec(memory_space=pl.ANY)


def near(array):
    return array if INTERPRET else pltpu.with_memory_space_constraint(array, pltpu.VMEM)


def far(array):
    return array if INTERPRET else pltpu.with_memory_space_constraint(array, pltpu.HBM)


def near_out(shape, kind):
    return jax.ShapeDtypeStruct(shape, kind) if INTERPRET else pltpu.VMEM(shape, kind)


def call(kernel, args, specs, outs, out_specs, scratch=(), flops=0, traffic=0, mib=16, **more):
    return pl.pallas_call(
        kernel,
        in_specs=specs,
        out_specs=out_specs,
        out_shape=outs,
        scratch_shapes=list(scratch),
        interpret=INTERPRET,
        compiler_params=pltpu.CompilerParams(vmem_limit_bytes=mib << 20),
        cost_estimate=pl.CostEstimate(flops=flops, bytes_accessed=traffic, transcendentals=0),
        **more,
    )(*args)


def load_kernel(source, out, sem):
    place = placement()
    depth = source.shape[1] // 2
    for pair, yh in itertools.product(range(source.shape[0]), range(2)):
        rows = slice(yh * depth, (yh + 1) * depth)
        used = 2 * pair + yh <= place[1]

        @pl.when(used)
        def _():
            pltpu.make_async_copy(source.at[pair, rows, :], out.at[pair, rows, :], sem.at[pair, yh]).start()

        @pl.when(jnp.logical_not(used))
        def _():
            out[pair, rows, :] = jnp.zeros((depth, source.shape[2]), out.dtype)

    for pair, yh in itertools.product(range(source.shape[0]), range(2)):
        rows = slice(yh * depth, (yh + 1) * depth)

        @pl.when(2 * pair + yh <= place[1])
        def _():
            pltpu.make_async_copy(source.at[pair, rows, :], out.at[pair, rows, :], sem.at[pair, yh]).wait()


def loaded(array):
    return call(
        load_kernel,
        [far(array)],
        [FAR],
        near_out(array.shape, array.dtype),
        CHIP,
        [pltpu.SemaphoreType.DMA((array.shape[0], 2))],
        flops=array.size * 400,
        traffic=array.size * 4,
        mib=1,
    )


def quarters(turn, quarter):
    first = slice(turn * quarter, (turn + 1) * quarter)
    second = slice((1 - turn) * quarter, (2 - turn) * quarter)
    return first, second


def lay_out_pair(a, b, lhs):
    quarter, latent = a.shape[1:]
    for i, (turn, x) in enumerate(ORDER):
        rows_a, rows_b = quarters(turn, quarter)
        for yh in range(2):
            at = 4 * x + 2 * yh
            lanes = slice((2 * i + yh) * latent, (2 * i + yh + 1) * latent)
            lhs[rows_a, lanes] = a[at + turn]
            lhs[rows_b, lanes] = b[at + 1 - turn]


def lay_out(place, offset, sides, lhs):
    half = lhs.shape[0] // len(sides)
    latent = sides[0][0].shape[2]
    for i, (turn, x) in enumerate(ORDER):
        rows_a, rows_b = quarters(turn, half // 2)
        for yh in range(2):
            layer = 2 * pair_of(place, offset, turn, x) + yh
            at = 4 * x + 2 * yh
            lanes = slice((2 * i + yh) * latent, (2 * i + yh + 1) * latent)

            @pl.when(layer <= place[1])
            def _():
                for side, (a, b) in enumerate(sides):
                    block = lhs.at[side * half : (side + 1) * half]
                    block[rows_a, lanes] = a[at + turn]
                    block[rows_b, lanes] = b[at + 1 - turn]

            @pl.when(layer > place[1])
            def _():
                lhs[:, lanes] = jnp.zeros((lhs.shape[0], latent), lhs.dtype)


def lay_out_block(block, lhs):
    quarter, latent = block.shape[1:]
    for q, x, yh in itertools.product(range(2), range(RING), range(2)):
        rows = slice(q * quarter, (q + 1) * quarter)
        lanes = slice((2 * x + yh) * latent, (2 * x + yh + 1) * latent)
        lhs[rows, lanes] = block[4 * x + 2 * yh + q]


def block_product(place, shift, lhs, source, cols):
    quarter = lhs.shape[0] // 2
    parts = []
    for q in range(2):
        pairs = [pair_of(place, shift, q, x) for x in range(RING)]
        rhs = jnp.concatenate([source[pair, :, cols] for pair in pairs], axis=0)
        rows = slice(q * quarter, (q + 1) * quarter)
        parts.append(jnp.dot(lhs[rows, :], rhs, preferred_element_type=f32))
    return jnp.concatenate(parts, axis=0)


def column_steps(columns):
    step = min(512, columns)
    for start in range(0, columns, step):
        yield start, slice(start, start + step)


def home_kernel(block, w, v, total, lhs):
    place = placement()
    lay_out_block(block, lhs)
    columns = w.shape[2]
    for side, source in enumerate((w, v)):
        for start, cols in column_steps(columns):
            both = slice(side * columns + start, side * columns + cols.stop)
            total[:, both] = block_product(place, 0, lhs, source, cols)


def rebuilt_home(block, w, v):
    quarter, latent = block.shape[1:]
    half = 2 * quarter
    depth, columns = w.shape[1:]
    args = [near(t) for t in (block, w, v)]
    scratch = [pltpu.VMEM((half, 8 * latent), bf16)]
    out = near_out((half, 2 * columns), f32)
    flops = half * 2 * columns * 8 * depth
    return call(home_kernel, args, [CHIP] * 3, out, CHIP, scratch, flops, 1 << 20)


def forward_kernel(tokens, two, a, b, w, v, before, outputs, other, *rest):
    place = placement()
    signal, signal_other, squares, lhs, lhs_two, wanted, wanted_other, sems = rest
    half = 2 * a.shape[1]
    columns = w.shape[2]
    rows = pl.ds(pl.multiple_of(place[2] * half, 16), half)
    copy = pltpu.make_async_copy(outputs.at[rows, :], wanted, sems.at[0])
    copy.start()
    copy_other = pltpu.make_async_copy(other, wanted_other, sems.at[1])
    copy_other.start()
    lay_out_block(two, lhs_two)
    lay_out_pair(a, b, lhs)
    pairs = [pair_of(place, 1, turn, x) for turn, x in ORDER]
    carry = jnp.zeros((16, 128), f32)
    sides = ((w, wanted, signal), (v, wanted_other, signal_other))
    for side, (source, target, out) in enumerate(sides):
        for start, cols in column_steps(columns):
            both = slice(side * columns + start, side * columns + cols.stop)
            rhs = jnp.concatenate([source[pair, :, cols] for pair in pairs], axis=0)
            product = jnp.dot(lhs[...], rhs, preferred_element_type=f32)
            product = product + block_product(place, 2, lhs_two, source, cols)
            if side == 0 and start == 0:
                copy.wait()
                copy_other.wait()
            misfit = product + before[:, both] - target[:, cols].astype(f32)
            out[:, cols] = (misfit * (1.0 / tokens)).astype(bf16)
            square = misfit * misfit
            square = jnp.sum(square.reshape(-1, 16, square.shape[1]), axis=0)
            for lane in range(0, square.shape[1], 128):
                carry = carry + square[:, lane : lane + 128]
    squares[...] = carry


def forward(tokens, two, a, b, w, v, before, outputs, wanted_other):
    quarter, latent = a.shape[1:]
    half = 2 * quarter
    depth, columns = w.shape[1:]
    args = [near(t) for t in (two, a, b, w, v, before)] + [far(outputs), wanted_other]
    specs = [CHIP] * 6 + [FAR, ANY]
    scratch = [pltpu.VMEM((half, 16 * latent), bf16), pltpu.VMEM((half, 8 * latent), bf16)]
    scratch += [pltpu.VMEM((half, columns), bf16)] * 2 + [pltpu.SemaphoreType.DMA((2,))]
    outs = (near_out((half, columns), bf16), near_out((half, columns), bf16), near_out((16, 128), f32))
    flops = 3 * half * 2 * columns * 8 * depth
    kernel = functools.partial(forward_kernel, tokens)
    return call(kernel, args, specs, outs, (CHIP,) * 3, scratch, flops, 1 << 20)


def write_notes(squares, fired, *blocks):
    quarter, latent = blocks[0].shape[1] - EXTRA, blocks[0].shape[2]
    loss = 0.5 * jnp.sum(squares[...]) + sparsity * jnp.sum(fired[...])
    loss = jnp.full((8, latent), loss, f32)
    high = loss.astype(bf16).astype(f32)
    note = jnp.concatenate([high, loss - high], axis=0).astype(bf16)
    for block in blocks:
        for tile in range(block.shape[0]):
            block[tile, quarter:, :] = note


NT = (((1,), (1,)), ((), ()))


def terms_kernel(offset, signal, signal_other, w, v, squares, fired, a, b):
    place = placement()
    quarter, latent = a.shape[1] - EXTRA, a.shape[2]
    write_notes(squares, fired, a, b)
    for turn in range(2):
        pairs = [pair_of(place, offset, turn, x) for x in range(RING)]
        rows_a, rows_b = quarters(turn, quarter)
        term = None
        for left, right in ((signal, w), (signal_other, v)):
            rhs = jnp.concatenate([right[pair] for pair in pairs], axis=0)
            part = lax.dot_general(left[...], rhs, NT, preferred_element_type=f32)
            term = part if term is None else term + part
        term = term.astype(bf16)
        for x, yh in itertools.product(range(RING), range(2)):
            at = 4 * x + 2 * yh
            lanes = slice((2 * x + yh) * latent, (2 * x + yh + 1) * latent)
            a[at + turn, :quarter, :] = term[rows_a, lanes]
            b[at + 1 - turn, :quarter, :] = term[rows_b, lanes]


def terms_for(offset, signal, signal_other, w, v, squares, fired):
    half, columns = signal.shape
    depth = w.shape[1]
    latent = depth // 2
    args = [near(t) for t in (signal, signal_other, w, v, squares, fired)]
    out = near_out((16, half // 2 + EXTRA, latent), bf16)
    flops = 2 * half * 2 * columns * 8 * depth
    kernel = functools.partial(terms_kernel, offset)
    return call(kernel, args, [CHIP] * 6, (out, out), (CHIP, CHIP), (), flops, 1 << 20)


def gradient_kernel(offset, a, b, a_other, b_other, signal, signal_other, *rest):
    place = placement()
    out, lhs, rhs, held, sems, sems_in = rest[-6:]
    half = signal.shape[0]
    depth = held.shape[1]
    incoming = pltpu.make_async_copy(signal, rhs.at[:half, :], sems_in.at[0])
    incoming.start()
    incoming_other = pltpu.make_async_copy(signal_other, rhs.at[half:, :], sems_in.at[1])
    incoming_other.start()
    lay_out(place, offset, [(a, b), (a_other, b_other)], lhs)
    incoming.wait()
    incoming_other.wait()
    contract = (((0,), (0,)), ((), ()))
    copies = []
    for i in range(0, len(ORDER), 2):
        left = lhs[:, i * depth : (i + 2) * depth]
        product = lax.dot_general(left, rhs[...], contract, preferred_element_type=f32).astype(bf16)
        for j in range(2):
            held[i + j] = product[j * depth : (j + 1) * depth]
            pair = pair_of(place, offset, *ORDER[i + j])
            copy = pltpu.make_async_copy(held.at[i + j], out.at[pair], sems.at[i + j])
            copy.start()
            copies.append(copy)
    for copy in copies:
        copy.wait()


def gradient(offset, a, b, a_other, b_other, signal, signal_other, so_far=None):
    latent = a.shape[2]
    half, columns = signal.shape
    args = [near(t) for t in (a, b, a_other, b_other)] + [signal, far(signal_other)]
    specs = [CHIP] * 4 + [ANY, FAR]
    aliases = {}
    if so_far is not None:
        aliases = {len(args): 0}
        args.append(so_far)
        specs.append(FAR)
    scratch = [
        pltpu.VMEM((2 * half, 16 * latent), bf16),
        pltpu.VMEM((2 * half, columns), bf16),
        pltpu.VMEM((len(ORDER), 2 * latent, columns), bf16),
        pltpu.SemaphoreType.DMA((len(ORDER),)),
        pltpu.SemaphoreType.DMA((2,)),
    ]
    out = jax.ShapeDtypeStruct((RING * RING, 2 * latent, columns), bf16)
    flops = 2 * 2 * half * columns * 16 * latent
    kernel = functools.partial(gradient_kernel, offset)
    return call(
        kernel, args, specs, out, FAR, scratch, flops, 1 << 20, mib=20, input_output_aliases=aliases
    )


def sum_kernel(own, one, two, three, out):
    quarter = own.shape[1] - EXTRA
    parts = (own, one, two, three)
    for tile in range(own.shape[0]):
        total = functools.reduce(lambda s, p: s + p, [p[tile, :quarter, :].astype(f32) for p in parts])
        out[tile, :quarter, :] = total.astype(bf16)
        row = lax.broadcasted_iota(jnp.int32, (EXTRA, own.shape[2]), 0)
        note = jnp.zeros((EXTRA, own.shape[2]), f32)
        for i, part in enumerate(parts):
            heard = part[tile, quarter:, :].astype(f32)
            high = jnp.broadcast_to(heard[:1], heard.shape)
            low = jnp.broadcast_to(heard[8:9], heard.shape)
            note = jnp.where(row == 2 * i, high, jnp.where(row == 2 * i + 1, low, note))
        out[tile, quarter:, :] = note.astype(bf16)


def summed(*parts):
    args = [near(part) for part in parts]
    out = near_out(parts[0].shape, bf16)
    return call(sum_kernel, args, [CHIP] * 4, out, CHIP, (), 1 << 20, 1 << 20, mib=4)


def encode_kernel(flip, inputs, weights, *rest):
    place = placement()
    out, rows_here, weights_here, bias_here, sems = rest[-5:]
    half = out.shape[0]
    which = 1 - place[2] if flip else place[2]
    rows = pl.ds(pl.multiple_of(which * half, 16), half)
    copies = [
        pltpu.make_async_copy(inputs.at[rows, :], rows_here, sems.at[0]),
        pltpu.make_async_copy(weights, weights_here, sems.at[1]),
    ]
    if not flip:
        copies.append(pltpu.make_async_copy(rest[0], bias_here, sems.at[2]))
    for copy in copies:
        copy.start()
    for copy in copies:
        copy.wait()
    out[...] = jnp.dot(rows_here[...], weights_here[...], preferred_element_type=f32)
    if not flip:

        @pl.when(place[3] == 0)
        def _():
            out[...] += bias_here[...]


def encoded(flip, inputs, weights, bias):
    tokens, columns = inputs.shape
    latent = weights.shape[1]
    scratch = [
        pltpu.VMEM((tokens // 2, columns), bf16),
        pltpu.VMEM((columns, latent), bf16),
        pltpu.VMEM((1, latent), f32),
        pltpu.SemaphoreType.DMA((3,)),
    ]
    out = near_out((tokens // 2, latent), f32)
    kernel = functools.partial(encode_kernel, flip)
    args = [far(inputs), far(weights)] + ([] if flip else [far(bias)])
    return call(kernel, args, [FAR] * len(args), out, CHIP, scratch, 1 << 20, 1 << 20, mib=4)


def fire_kernel(mine, heard, fired, blocks):
    place = placement()
    quarter = heard.shape[0]
    rows = pl.ds(pl.multiple_of(place[3] * quarter, 16), quarter)
    value = mine[rows, :] + heard[...]
    active = jnp.maximum(value, 0.0)
    fired[...] = jnp.sum(active.reshape(-1, 8, active.shape[1]), axis=0)
    firing = active.astype(bf16)
    for tile in range(blocks.shape[0]):
        blocks[tile] = firing


def fire(mine, heard):
    quarter, latent = heard.shape
    args = [near(mine), near(heard)]
    outs = (
        near_out((8, latent), f32),
        near_out((16, quarter, latent), bf16),
    )
    return call(fire_kernel, args, [CHIP] * 2, outs, (CHIP,) * 2, (), 1 << 20, 1 << 20, mib=4)


def delta_kernel(tokens, arrived, firing, delta):
    place = placement()
    quarter, latent = firing.shape[1:]
    total = arrived[0, :quarter, :].astype(f32)
    for tile in range(1, arrived.shape[0]):
        total = total + arrived[tile, :quarter, :].astype(f32)
    positive = firing[place[4]].astype(f32) > 0
    total = jnp.where(positive, total + sparsity / tokens, 0.0)
    delta[:quarter, :] = total.astype(bf16)
    losses = []
    for tile in range(arrived.shape[0]):
        notes = arrived[tile, quarter:, :].astype(f32)
        losses += [notes[2 * i : 2 * i + 1] + notes[2 * i + 1 : 2 * i + 2] for i in range(RING)]
    losses = jnp.concatenate(losses, axis=0)
    unit = jnp.maximum(jnp.max(losses, axis=0, keepdims=True), 1e-30)
    whole = jnp.sum(jnp.round(losses * (65536.0 / unit)), axis=0, keepdims=True)
    loss = jnp.broadcast_to(whole * (unit / 65536.0), (8, latent))
    high = loss.astype(bf16).astype(f32)
    delta[quarter:, :] = jnp.concatenate([high, loss - high], axis=0).astype(bf16)


def delta_of(arrived, firing, tokens):
    quarter, latent = firing.shape[1:]
    args = [near(arrived), near(firing)]
    out = near_out((quarter + EXTRA, latent), bf16)
    kernel = functools.partial(delta_kernel, tokens)
    return call(kernel, args, [CHIP] * 2, out, CHIP, (), 1 << 20, 1 << 20, mib=8)


def finish_kernel(size, inputs, own, beside, opposite, last, encoder, bias, mean, delta):
    place = placement()
    quarter = own.shape[0] - EXTRA
    core, side = place[2], place[3]
    parts = ((own, core, side), (beside, core, 1 - side), (opposite, 1 - core, side), (last, 1 - core, 1 - side))
    for part, c, y in parts:
        delta[pl.ds(pl.multiple_of((2 * c + y) * quarter, 16), quarter), :] = part[:quarter, :]
    contract = (((0,), (0,)), ((), ()))
    product = lax.dot_general(inputs[...], delta[...], contract, preferred_element_type=f32)
    encoder[...] = product.astype(bf16)
    bias[...] = jnp.sum(delta[...].astype(f32), axis=0, keepdims=True)
    losses = []
    for part in (own, opposite):
        notes = part[quarter:, :].astype(f32)
        losses.append(jnp.max(notes[:8] + notes[8:]))
    mean[0, 0] = (losses[0] + losses[1]) / size


def finished(size, inputs, *parts):
    tokens, columns = inputs.shape
    latent = parts[0].shape[1]
    args = [near(t) for t in (inputs, *parts)]
    outs = (
        jax.ShapeDtypeStruct((columns, latent), bf16),
        jax.ShapeDtypeStruct((1, latent), f32),
        jax.ShapeDtypeStruct((1, 1), f32),
    )
    scratch = [pltpu.VMEM((tokens, latent), bf16)]
    kernel = functools.partial(finish_kernel, size)
    return call(
        kernel, args, [CHIP] * 5, outs, (CHIP, CHIP, SCALARS), scratch, 1 << 20, 1 << 20, mib=8
    )


def whole_step(mlp_inputs, mlp_outputs, encoders, encoder_bias, decoders):
    inputs = mlp_inputs[0]
    tokens = inputs.shape[0]
    width = inputs.shape[1] * lax.axis_size(WIDTH)
    layers = lax.axis_size(LAYER)
    latent = encoders.shape[2]
    core = lax.axis_index("c")

    theirs = encoded(True, inputs, encoders[0], encoder_bias)
    heard = swapped(theirs, "c")
    mine = encoded(False, inputs, encoders[0], encoder_bias)
    weights = decoders[0].reshape(layers // 2, 2 * latent, -1)
    outputs = mlp_outputs[0]
    heard, weights, outputs = lax.optimization_barrier((heard, weights, outputs))
    partial = mine + heard
    weights_other = swapped(weights, "c")
    _, theirs = halves(partial, "yl")
    half = tokens // 2
    wanted_sent = lax.dynamic_slice_in_dim(outputs, (1 - core) * half, half, 0)
    wanted_other = swapped(wanted_sent, "c")
    heard = swapped(theirs, "yl")
    fired, blocks = fire(partial, heard)

    own = in_coset(blocks)
    two = sent(own, 2)
    one = sent(own, 1)
    three = sent(own, 3)
    own_other = swapped(own, "c")
    two_other = swapped(two, "c")
    one_other = swapped(one, "c")
    three_other = swapped(three, "c")

    weights = loaded(weights)
    weights_other = loaded(weights_other)
    total = rebuilt_home(own, weights, weights_other)
    signal, signal_other, squares = forward(
        tokens, two, three, one, weights, weights_other, total, outputs, wanted_other
    )
    signal_here = swapped(signal_other, "c")

    rest = (signal, signal_other, weights, weights_other, squares, fired)
    at_home, to_two = terms_for(0, *rest)
    from_two = sent(to_two, 2, back=True)
    to_three, to_one = terms_for(1, *rest)
    from_one = sent(to_one, 1, back=True)
    from_three = sent(to_three, 3, back=True)
    signals = (signal, signal_here)
    grad_decoder = gradient(0, own, two, own_other, two_other, *signals)
    arrived = in_coset(summed(at_home, from_one, from_two, from_three))
    grad_decoder = gradient(1, three, one, three_other, one_other, *signals, grad_decoder)

    delta = delta_of(arrived, own, tokens)
    beside = swapped(delta, "yl")
    last = lax.ppermute(delta, WIDTH, [(0, 3), (1, 2), (2, 1), (3, 0)])
    opposite = swapped(delta, "c")
    size = float(tokens * width * layers)
    grad_encoder, grad_bias, loss_mean = finished(
        size, inputs, delta, beside, opposite, last
    )
    return (loss_mean[0, 0], grad_encoder[None], grad_bias, grad_decoder.reshape(decoders.shape))


def solution(mesh):
    finer = Mesh(mesh.devices.reshape(4, 4, 2, 2, 2), AXES)
    placed = (
        P(LAYER, None, WIDTH),
        P(LAYER, None, WIDTH),
        P(LAYER, WIDTH, None),
        P(LAYER, None),
        P(LAYER, None, None, WIDTH),
    )
    return jax.shard_map(
        whole_step,
        mesh=finer,
        in_specs=placed,
        out_specs=(P(), P(LAYER, WIDTH, None), P(LAYER, None), P(LAYER, None, None, WIDTH)),
        check_vma=False,
    )
```
